32 devices in a mesh: member: 4 (over y, x), grid: 8 (over z, core).
Axes of the slice: x: 2, y: 2, z: 4, core: 2. Of those that a mesh axis runs over, the one named last changes fastest.
Arguments:
- prior_ensemble: bfloat16 [40, 48, 32768], P('member', None, 'grid'), may hold values from -6 to 6
- domain_site_mapping: int32 [8, 4, 1024], P(None, None, 'grid'), may hold values from 0 to 4095, as said below
- neighbour_triples: int32 [8, 3, 4096], P('grid', None, 'member'), may hold values from 0 to 159
- stencil_factors: float32 [8, 3, 4096], P('grid', None, 'member'), may hold values from 0.1 to 1
- sparse_node_transforms: float32 [1600, 1024], P(None, 'grid'), may hold values from -0.4 to 1.8
Outputs:
- analysis: bfloat16 [40, 48, 32768], P('member', None, 'grid')
The draws below stay inside these ranges and needn't reach their ends.
Inputs may be any that keep to these rules, and one draw needn't show every extreme that they name: For every model patch h, the entries domain_site_mapping[:, :, h * 128 : (h + 1) * 128] hold every number from 0 to 4095 exactly once.
All inputs are finite; a program needn't handle non-finite values.
Results may differ from the reference program's by a relative error of at most 0.0076.
Values may be sent and summed in bfloat16 or wider, within the bound.
A program may use at most 128 MiB of HBM per device.

```python
import math
import jax
import jax.numpy as jnp
from jax import lax

ENSEMBLE_SIZE = 40
STATE_QUANTITIES = 48
CELLS_DEV = 4096
COARSE_DEV = 128
RIM = 16
PATCHES = 8
GROUPS = 4
COLUMNS = 1024
PER_SOURCE = 128
MESH_SITES = 32768
COARSE = 1024


def draw_domain_site_mapping(key, part):
    subkeys = jax.random.split(jax.random.fold_in(key, 11), PATCHES)
    shuffled = jax.vmap(lambda subkey: jax.random.permutation(subkey, CELLS_DEV))(subkeys)
    shuffled = shuffled.reshape(PATCHES, PATCHES, GROUPS, PER_SOURCE)
    return jnp.transpose(shuffled, (1, 2, 0, 3)).reshape(PATCHES, GROUPS, COLUMNS).astype(jnp.int32)


def draw_sparse_node_transforms(key, part):
    first_key = jax.random.fold_in(key, 21)
    second_key = jax.random.fold_in(key, 22)
    scatter_part = jnp.clip(0.12 * jax.random.normal(first_key, (ENSEMBLE_SIZE, ENSEMBLE_SIZE, COARSE), jnp.float32), -0.4, 0.4)
    diagonal_part = jax.random.uniform(second_key, (ENSEMBLE_SIZE, COARSE), jnp.float32, 0.6, 1.4)
    weights = scatter_part + jnp.eye(ENSEMBLE_SIZE, dtype=jnp.float32)[:, :, None] * diagonal_part[:, None, :]
    return weights.reshape(ENSEMBLE_SIZE * ENSEMBLE_SIZE, COARSE).astype(jnp.float32)


def place_ends(drawn, stream_key, smallest, high):
    spot = [jax.random.randint(jax.random.fold_in(stream_key, axis), (), 0, length) for axis, length in enumerate(drawn.shape)]
    widest = drawn.shape.index(max(drawn.shape))
    next_to = spot[:widest] + [(spot[widest] + 1) % drawn.shape[widest]] + spot[widest + 1:]
    return drawn.at[tuple(spot)].set(smallest).at[tuple(next_to)].set(high)


def shard_levels(rng, dims, cuts, low, top_value):
    factor_of = 1.0
    for dim, parts in cuts:
        steps = jax.random.uniform(jax.random.fold_in(jax.random.fold_in(rng, 6), dim), (parts,), jnp.float32, low / len(cuts), top_value / len(cuts))
        factor_of = factor_of * jnp.repeat(jnp.exp(steps), dims[dim] // parts).reshape((-1,) + (1,) * (len(dims) - 1 - dim))
    return factor_of


def scatter_about(stream_key, shape, scale, limit, pieces=(), kind=jnp.bfloat16):
    gain = shard_levels(stream_key, shape, pieces, -0.22, 0.18) if pieces else 1.0
    entries = jax.random.normal(stream_key, shape, jnp.float32) * scale * gain
    return jnp.minimum(jnp.maximum(entries, -limit), limit).astype(kind)


def setup_inputs(seed: int = 0) -> dict:
    seeds = jax.random.split(jax.random.key(seed), 6)
    return {
        "prior_ensemble": scatter_about(seeds[0], (ENSEMBLE_SIZE, STATE_QUANTITIES, MESH_SITES), 1.0, 6.0, ((0, 4), (2, 8))),
        "domain_site_mapping": draw_domain_site_mapping(jax.random.fold_in(seeds[5], 71), 0),
        "neighbour_triples": place_ends(jax.random.randint(seeds[2], (PATCHES, 3, CELLS_DEV), 0, COARSE_DEV + 2 * RIM), jax.random.fold_in(seeds[2], 1), 0, (COARSE_DEV + 2 * RIM) - 1).astype(jnp.int32),
        "stencil_factors": jnp.clip(jnp.exp(math.log(1.0) - 2.3025851 * jax.random.uniform(seeds[3], (PATCHES, 3, CELLS_DEV), jnp.float32) ** shard_levels(seeds[3], (PATCHES, 3, CELLS_DEV), ((0, 8), (2, 4)), -0.2, 0.2)), 0.1, 1.0),
        "sparse_node_transforms": draw_sparse_node_transforms(jax.random.fold_in(seeds[5], 71), 0),
    }


def reference(prior_ensemble, domain_site_mapping, neighbour_triples, stencil_factors, sparse_node_transforms):
    source_base = (jnp.arange(COLUMNS, dtype=jnp.int32) // PER_SOURCE) * CELLS_DEV
    cell_ids = (domain_site_mapping + source_base[None, None, :]).reshape(PATCHES, CELLS_DEV).astype(jnp.int32)

    def one_patch(inputs):
        sites_within_tile, points, raw_share, patch_id = inputs
        arriving_analysis_slots = jnp.take(prior_ensemble, sites_within_tile, axis=2)
        member_mean = jnp.sum(arriving_analysis_slots, axis=0, dtype=jnp.float32) / ENSEMBLE_SIZE
        deviation = (arriving_analysis_slots.astype(jnp.float32) - member_mean[None]).astype(jnp.bfloat16)
        coarse_ids = ((patch_id * COARSE_DEV - RIM + points) % COARSE).astype(jnp.int32)
        shares = raw_share / jnp.sum(raw_share, axis=0, keepdims=True)
        blended = jnp.zeros((ENSEMBLE_SIZE * ENSEMBLE_SIZE, CELLS_DEV), jnp.float32)
        for which in range(3):
            blended = blended + jnp.take(sparse_node_transforms, coarse_ids[which], axis=1) * shares[which][None, :]
        blended = blended.reshape(ENSEMBLE_SIZE, ENSEMBLE_SIZE, CELLS_DEV).astype(jnp.bfloat16)
        result = jnp.einsum('kfc,kjc->jfc', deviation.astype(jnp.float32), blended.astype(jnp.float32)) + member_mean[None]
        return result.astype(jnp.bfloat16)

    patch_list = jnp.arange(PATCHES, dtype=jnp.int32)
    results = lax.map(one_patch, (cell_ids, neighbour_triples, stencil_factors, patch_list))
    ordered = jnp.moveaxis(results, 0, 2).reshape(ENSEMBLE_SIZE, STATE_QUANTITIES, MESH_SITES)
    analysis = jnp.zeros((ENSEMBLE_SIZE, STATE_QUANTITIES, MESH_SITES), jnp.bfloat16)
    analysis = analysis.at[:, :, cell_ids.reshape(-1)].set(ordered)
    return analysis
```

```python
import functools

import jax
import jax.numpy as jnp
from jax import lax
from jax.experimental import pallas as pl
from jax.experimental.pallas import tpu as pltpu
from jax.sharding import PartitionSpec as P

RIM = 16
DIGIT = 128
CHUNKS = 2


def update_kernel(ids_ref, share_ref, t_ref, x_ref, out_ref, w_ref, dev_ref, mean_ref, acc_ref):
    members, fields, width = x_ref.shape
    pairs, coarse = t_ref.shape
    slots = lax.broadcasted_iota(jnp.int32, (coarse, width), 0)
    spread = jnp.zeros((coarse, width), jnp.float32)
    for s in range(3):
        spread = spread + jnp.where(ids_ref[s : s + 1, :] == slots, share_ref[s : s + 1, :], 0.0)
    spread = spread.astype(jnp.bfloat16)
    rows = pairs // 10

    def blend(i, carry):
        at = pl.ds(pl.multiple_of(i * rows, rows), rows)
        part = jnp.dot(t_ref[at, :], spread, preferred_element_type=jnp.float32)
        w_ref[pl.ds(i * (rows // 8), rows // 8)] = part.reshape(rows // 8, 8, width)
        return carry

    lax.fori_loop(0, 10, blend, 0)

    def add(k, total):
        return total + x_ref[k].astype(jnp.float32)

    mean_ref[...] = (
        lax.fori_loop(0, members, add, jnp.zeros((fields, width), jnp.float32)) / members
    )

    def center(k, carry):
        d = x_ref[k].astype(jnp.float32) - mean_ref[...]
        dev_ref[k] = d.astype(jnp.bfloat16).astype(jnp.float32)
        return carry

    lax.fori_loop(0, members, center, 0)
    group = 8
    unroll = 8
    half = fields // 2
    for lane in range(0, width, 128):
        lanes = slice(lane, lane + 128)
        for field in (0, half):
            some_fields = slice(field, field + half)

            def contract(jg, carry, lanes=lanes, some_fields=some_fields):
                def some(kk, accs):
                    accs = list(accs)
                    for u in range(unroll):
                        k = kk * unroll + u
                        d = dev_ref[k, some_fields, lanes]
                        for jj in range(group):
                            w = w_ref[k * (members // group) + jg, jj : jj + 1, lanes]
                            accs[jj] = accs[jj] + d * w
                    return tuple(accs)

                first = tuple(mean_ref[some_fields, lanes] for _ in range(group))
                accs = lax.fori_loop(0, members // unroll, some, first)
                for jj in range(group):
                    acc_ref[jg * group + jj, some_fields, lanes] = accs[jj]
                return carry

            lax.fori_loop(0, members // group, contract, 0)
    lax.fori_loop(0, members, lambda j, c: store(j, c, out_ref, acc_ref), 0)


def store(j, carry, out_ref, acc_ref):
    out_ref[j] = acc_ref[j].astype(jnp.bfloat16)
    return carry


def update(ids, shares, transforms, gathered):
    members, fields, columns = gathered.shape
    pairs, coarse = transforms.shape
    width = min(256, columns)
    flops = 2 * pairs * columns * (coarse + 8 * fields)
    return pl.pallas_call(
        update_kernel,
        grid=(columns // width,),
        out_shape=jax.ShapeDtypeStruct(gathered.shape, jnp.bfloat16),
        in_specs=[
            pl.BlockSpec((3, width), lambda i: (0, i)),
            pl.BlockSpec((3, width), lambda i: (0, i)),
            pl.BlockSpec((pairs, coarse), lambda i: (0, 0)),
            pl.BlockSpec((members, fields, width), lambda i: (0, 0, i)),
        ],
        out_specs=pl.BlockSpec((members, fields, width), lambda i: (0, 0, i)),
        scratch_shapes=[
            pltpu.VMEM((pairs // 8, 8, width), jnp.float32),
            pltpu.VMEM((members, fields, width), jnp.float32),
            pltpu.VMEM((fields, width), jnp.float32),
            pltpu.VMEM((members, fields, width), jnp.float32),
        ],
        compiler_params=pltpu.CompilerParams(vmem_limit_bytes=62 * 1024 * 1024),
        cost_estimate=pl.CostEstimate(flops=flops, bytes_accessed=12_000_000, transcendentals=0),
    )(ids, shares, transforms, gathered)


def assemble_kernel(*refs):
    out_ref = refs[-1]
    part = refs[0].shape[3]

    def put(k, carry):
        for i, ref in enumerate(refs[:-1]):
            out_ref[k, :, i * part : (i + 1) * part] = ref[0, k]
        return carry

    lax.fori_loop(0, out_ref.shape[0], put, 0)


def assemble(results):
    groups, members, fields, part = results[0].shape
    width = part * len(results)
    return pl.pallas_call(
        assemble_kernel,
        grid=(groups,),
        out_shape=jax.ShapeDtypeStruct((members, fields, groups * width), results[0].dtype),
        in_specs=[pl.BlockSpec((1, members, fields, part), lambda i: (i, 0, 0, 0))] * len(results),
        out_specs=pl.BlockSpec((members, fields, width), lambda i: (0, 0, i)),
    )(*results)


def on_device(prior, mapping, triples, factors, transforms):
    groups = lax.axis_size("member")
    patches = lax.axis_size("grid")
    cells = prior.shape[2]
    columns = cells // groups
    per_source = columns // patches
    coarse_dev = transforms.shape[1]
    coarse = coarse_dev * patches

    everywhere = lax.all_gather(transforms.astype(jnp.bfloat16), "grid", axis=1, tiled=True)

    region = lax.axis_index("grid")
    ids = (region * coarse_dev - RIM + triples[0] + coarse) % coarse
    raw = factors[0]
    shares = raw / jnp.sum(raw, axis=0, keepdims=True)
    table = jnp.concatenate(
        [
            (ids // DIGIT).astype(jnp.bfloat16),
            (ids % DIGIT).astype(jnp.bfloat16),
            shares.astype(jnp.bfloat16),
        ],
        axis=0,
    )
    table = jnp.transpose(table.reshape(9, patches, per_source), (1, 0, 2))
    table = jnp.broadcast_to(table[None], (groups, patches, 9, per_source))
    table = table.reshape(groups * patches, 9, per_source)
    part = columns // CHUNKS
    exchanged = []
    for chunk in range(CHUNKS):
        starts = [m * columns + chunk * part for m in range(groups)]
        blocks = jnp.stack([prior[:, :, at : at + part] for at in starts])
        exchanged.append(
            lax.all_to_all(blocks, "member", split_axis=0, concat_axis=0, tiled=True)
        )
    table = lax.all_to_all(table, ("member", "grid"), split_axis=0, concat_axis=0, tiled=True)
    table = jnp.transpose(table, (1, 0, 2)).reshape(9, cells)
    spots = jnp.transpose(mapping, (1, 0, 2)).reshape(cells)
    mine = lax.axis_index("member") * columns + jnp.arange(columns, dtype=jnp.int32)
    onehot = (spots[:, None] == mine[None, :]).astype(jnp.bfloat16)
    found = jnp.dot(table, onehot, preferred_element_type=jnp.float32)
    cell_ids = (found[0:3] * DIGIT + found[3:6]).astype(jnp.int32)
    cell_shares = found[6:9]

    results = []
    for chunk in range(CHUNKS):
        here = slice(chunk * part, (chunk + 1) * part)
        blocks = exchanged[chunk]
        gathered = blocks.reshape((-1,) + blocks.shape[2:])
        result = update(cell_ids[:, here], cell_shares[:, here], everywhere, gathered)
        result = result.reshape(blocks.shape)
        results.append(
            lax.all_to_all(result, "member", split_axis=0, concat_axis=0, tiled=True)
        )
    return assemble(results)


def solution(mesh):
    return jax.shard_map(
        on_device,
        mesh=mesh,
        in_specs=(
            P("member", None, "grid"),
            P(None, None, "grid"),
            P("grid", None, "member"),
            P("grid", None, "member"),
            P(None, "grid"),
        ),
        out_specs=P("member", None, "grid"),
        check_vma=False,
    )
```
